32 devices in a mesh: rep: 1, dp: 32 (over x, y, z, core).
Axes of the slice: x: 2, y: 2, z: 4, core: 2. Of those that a mesh axis runs over, the one named last changes fastest.
Arguments:
- x: bfloat16 [32, 2048, 896], P(('rep', 'dp'))
- dy: bfloat16 [32, 2048, 896], P(('rep', 'dp'))
- w_gate: bfloat16 [2, 896, 2560], replicated
- w_up: bfloat16 [2, 896, 2560], replicated
- w_down: bfloat16 [2, 2560, 896], replicated
- m_w_gate: float32 [2, 896, 2560], P(None, 'dp')
- m_w_up: float32 [2, 896, 2560], P(None, 'dp')
- m_w_down: float32 [2, 2560, 896], P(None, 'dp')
- v_w_gate: float32 [2, 896, 2560], P(None, 'dp')
- v_w_up: float32 [2, 896, 2560], P(None, 'dp')
- v_w_down: float32 [2, 2560, 896], P(None, 'dp')
Outputs:
- output 1: bfloat16 [2, 896, 2560], P('rep')
- output 2: bfloat16 [2, 896, 2560], P('rep')
- output 3: bfloat16 [2, 2560, 896], P('rep')
- output 4: float32 [2, 896, 2560], P('rep', 'dp')
- output 5: float32 [2, 896, 2560], P('rep', 'dp')
- output 6: float32 [2, 2560, 896], P('rep', 'dp')
- output 7: float32 [2, 896, 2560], P('rep', 'dp')
- output 8: float32 [2, 896, 2560], P('rep', 'dp')
- output 9: float32 [2, 2560, 896], P('rep', 'dp')
All inputs are finite; a program needn't handle non-finite values.
Results may differ from the reference program's by a relative error of at most 0.02.
Values are sent between devices in bfloat16 or wider.
A program may use at most 2 GiB of HBM per device.

```python
import jax
import jax.numpy as jnp
from jax import lax

SEQUENCES = 32
TOKENS = 2048
D = 896
FF = 2560
LAYERS = 2
NAMES = ("w_gate", "w_up", "w_down")
SHAPES = {"w_gate": (LAYERS, D, FF), "w_up": (LAYERS, D, FF), "w_down": (LAYERS, FF, D)}


def bump(key, n, height):
    away = (jnp.arange(n, dtype=jnp.int32) - jax.random.randint(key, (), 0, n, jnp.int32)) % n
    return jnp.where(away < n // 8, height, 1.0)


def together(key, own, strength):
    shared = jax.random.normal(key, own.shape[1:], jnp.float32)
    return (own + strength * shared) * lax.rsqrt(1 + strength * strength)


def setup_inputs(seed: int = 0, part: int = 0) -> dict:
    kx, kdy, ka, kb, kz, kf, kh, kl, *keys = jax.random.split(jax.random.key(seed), 8 + 3 * len(NAMES))
    kx, kdy, ka, kb = (jax.random.fold_in(k, part) for k in (kx, kdy, ka, kb))
    kw, km, kv = (keys[i::3] for i in range(3))
    shape = (SEQUENCES, TOKENS, D)
    much_x, much_dy = jax.random.uniform(kz, (2,), jnp.float32, 0.0, 1.0)
    loud = 2.0 ** jax.random.uniform(jax.random.fold_in(kz, 1), (), jnp.float32, -1.0, 2.0)
    layers = 2.0 ** jax.random.uniform(kl, (LAYERS, 1, 1), jnp.float32, -1.0, 1.0)
    x = together(ka, jax.random.normal(kx, shape, jnp.float32), much_x) * bump(kf, D, 4.0)
    dy = together(kb, jax.random.normal(kdy, shape, jnp.float32), much_dy)
    drawn = {"x": x.astype(jnp.bfloat16), "dy": (loud * dy * (SEQUENCES * TOKENS) ** -0.5).astype(jnp.bfloat16)}
    for key, name in zip(kw, NAMES, strict=True):
        w = jax.random.normal(key, SHAPES[name], jnp.float32) * SHAPES[name][1] ** -0.5
        drawn[name] = (w * {"w_gate": 1.0, "w_up": bump(kh, FF, 4.0), "w_down": layers}[name]).astype(jnp.bfloat16)
    for key, name in zip(km, NAMES, strict=True):
        drawn[f"m_{name}"] = 0.1 * jax.random.normal(key, SHAPES[name], jnp.float32)
    for key, name in zip(kv, NAMES, strict=True):
        drawn[f"v_{name}"] = jax.random.uniform(key, SHAPES[name], jnp.float32, 0.005, 0.015)
    return drawn


def matmul(a, w):
    return jnp.dot(a, w, preferred_element_type=jnp.float32).astype(jnp.bfloat16)


def normed(h):
    wide = h.astype(jnp.float32)
    scale = lax.rsqrt(jnp.mean(wide**2, -1, keepdims=True) + 1e-6)
    return (wide * scale).astype(jnp.bfloat16)


def layer(h, w):
    a = normed(h)
    gate = jnp.dot(a, w["w_gate"], preferred_element_type=jnp.float32)
    up = jnp.dot(a, w["w_up"], preferred_element_type=jnp.float32)
    return h + matmul((jax.nn.silu(gate) * up).astype(jnp.bfloat16), w["w_down"])


def adamw(w, m, v, g):
    m = 0.9 * m + 0.1 * g
    v = 0.95 * v + 0.05 * g * g
    step = m * lax.rsqrt(v + 1e-8) + 0.1 * w
    return (w - 0.02 * step).astype(jnp.bfloat16), m, v


def stack(weights, h):
    return lax.scan(lambda h, w: (layer(h, w), None), h, weights)[0]


def reference(x, dy, w_gate, w_up, w_down, m_w_gate, m_w_up, m_w_down, v_w_gate, v_w_up, v_w_down):
    weights = dict(zip(NAMES, (w_gate, w_up, w_down), strict=True))

    def take(so_far, sequence):
        h, by_y = sequence
        _, back = jax.vjp(lambda w: stack(w, h), weights)
        return jax.tree.map(lambda total, term: total + term.astype(jnp.float32), so_far, back(by_y)[0]), None

    none_yet = {name: jnp.zeros(w.shape, jnp.float32) for name, w in weights.items()}
    by_weights, _ = lax.scan(take, none_yet, (x, dy))
    gradients = [by_weights[name].astype(jnp.bfloat16).astype(jnp.float32) for name in NAMES]
    new = [
        adamw(w.astype(jnp.float32), m, v, g)
        for w, m, v, g in zip((w_gate, w_up, w_down), (m_w_gate, m_w_up, m_w_down), (v_w_gate, v_w_up, v_w_down), gradients, strict=True)
    ]
    return tuple(one[which] for which in range(3) for one in new)
```

```python
import functools

import jax
import jax.numpy as jnp
from jax import lax
from jax.experimental import pallas as pl
from jax.experimental.pallas import tpu as pltpu
from jax.sharding import PartitionSpec as P

F32, BF = jnp.float32, jnp.bfloat16
MESH = pl.DeviceIdType.MESH
WIDE, TALL = (32, 2560), (80, 896)


def dot(a, b, ca, cb):
    return lax.dot_general(a, b, (((ca,), (cb,)), ((), ())), preferred_element_type=F32)


def normed(h):
    wide = h.astype(F32)
    scale = lax.rsqrt(jnp.mean(wide**2, -1, keepdims=True) + 1e-6)
    return (wide * scale).astype(BF), scale


def spread():
    f, c = lax.broadcasted_iota(jnp.int32, (896, 1024), 0), lax.broadcasted_iota(jnp.int32, (896, 1024), 1)
    return (32 * (f // 28) + f % 28 == c).astype(BF)


def act_back(dp, g, u):
    s = jax.nn.sigmoid(g)
    dp = dp.astype(F32)
    return (dp * u * (s * (1 + g * (1 - s)))).astype(BF), (dp * g * s).astype(BF)


def gradients(x, dy, wg, wu, wd):
    place = spread()
    a0, _ = normed(x)
    g0, u0 = dot(a0, wg[0], 1, 0), dot(a0, wu[0], 1, 0)
    p0 = (jax.nn.silu(g0) * u0).astype(BF)
    h1 = x + dot(p0, wd[0], 1, 0).astype(BF)
    a1, s1 = normed(h1)
    g1, u1 = dot(a1, wg[1], 1, 0), dot(a1, wu[1], 1, 0)
    p1 = (jax.nn.silu(g1) * u1).astype(BF)
    dwd1 = dot(p1, dy, 0, 0).astype(BF)
    dg1, du1 = act_back(dot(dy, wd[1], 1, 1).astype(BF), g1, u1)
    b1 = dot(a1, place, 1, 0).astype(BF)
    dwg1, dwu1 = dot(b1, dg1, 0, 0).astype(BF), dot(b1, du1, 0, 0).astype(BF)
    da1 = dot(dg1, wg[1], 1, 1) + dot(du1, wu[1], 1, 1)
    unit = h1.astype(F32) * s1
    dh1 = dy + (s1 * (da1 - unit * jnp.mean(da1 * unit, -1, keepdims=True))).astype(BF)
    dwd0 = dot(p0, dh1, 0, 0).astype(BF)
    dg0, du0 = act_back(dot(dh1, wd[0], 1, 1).astype(BF), g0, u0)
    b0 = dot(a0, place, 1, 0).astype(BF)
    dwg0, dwu0 = dot(b0, dg0, 0, 0).astype(BF), dot(b0, du0, 0, 0).astype(BF)
    return dwd1, dwg1, dwu1, dwd0, dwg0, dwu0


CHUNKS = [(TALL, 2, 1), (WIDE, 0, 1), (WIDE, 1, 1), (TALL, 2, 0), (WIDE, 0, 0), (WIDE, 1, 0)]


def exchange(*refs):
    n = len(CHUNKS)
    grads, ws, ms, vs = refs[:n], refs[n : n + 3], refs[n + 3 : n + 6], refs[n + 6 : n + 9]
    outs, mo, vo = refs[n + 9 : 2 * n + 9], refs[2 * n + 9 : 2 * n + 12], refs[2 * n + 12 : 2 * n + 15]
    scratch = refs[2 * n + 15 :]
    own, r0, r1, r2, r3, new = (scratch[i * n : (i + 1) * n] for i in range(6))
    local_sem, send_sem, recv_sem = scratch[6 * n :]

    me = lax.axis_index("dp")
    c, z, y, x = me % 2, (me // 2) % 4, (me // 8) % 2, me // 16
    core, px, py = me + 1 - 2 * c, me + 16 - 32 * x, me + 8 - 16 * y
    pz = [me + 2 * ((z + d) % 4 - z) for d in (1, 2, 3)]

    barrier = pltpu.get_barrier_semaphore()
    for peer in (core, px, py, *pz):
        pl.semaphore_signal(barrier, inc=1, device_id={"dp": peer}, device_id_type=MESH)
    pl.semaphore_wait(barrier, 6)

    def remote(k, slot, src, dst, peer):
        return pltpu.make_async_remote_copy(
            src_ref=src, dst_ref=dst, send_sem=send_sem.at[k, slot], recv_sem=recv_sem.at[k, slot],
            device_id={"dp": peer}, device_id_type=MESH,
        )

    def rows(k, blocks, body):
        per = CHUNKS[k][0][0] // 16

        def step(i, _):
            body(i // per, pl.ds(pl.multiple_of(i % per * 16, 16), 16))
            return 0

        lax.fori_loop(0, blocks * per, step, 0)

    def wide(ref, *at):
        return ref[at].astype(F32)

    sent = []

    def go(copy):
        copy.start()
        sent.append(copy)
        return copy

    stages = [{} for _ in range(n)]
    for k in range(n):
        stages[k]["own"] = pltpu.make_async_copy(grads[k].at[:, :, :, :, c], own[k], local_sem.at[k, 0])
        stages[k]["own"].start()
        stages[k]["core"] = go(remote(k, 0, grads[k].at[:, :, :, :, 1 - c], r0[k], core))

    for k in range(n):
        stages[k]["own"].wait()
        stages[k]["core"].wait_recv()

        def first(i, r, k=k):
            q, zz = i // 2, i % 2
            at = (1 - x, q, 0, zz, r)
            r0[k][at] = (wide(r0[k], *at) + wide(own[k], *at)).astype(BF)

        rows(k, 4, first)
        stages[k]["a1"] = go(remote(k, 1, r0[k].at[1 - x, :, 0], r1[k].at[0], px))

        def second(i, r, k=k):
            q, zz = i // 2, i % 2
            at = (q, 1 - y, 1, zz, r)
            r0[k][at] = (wide(r0[k], *at) + wide(own[k], *at)).astype(BF)

        rows(k, 4, second)
        stages[k]["b1"] = go(remote(k, 2, r0[k].at[:, 1 - y, 1], r1[k].at[1], py))

    for k in range(n):
        stages[k]["a1"].wait_recv()

        def first(zz, r, k=k):
            at = (x, 1 - y, 0, zz, r)
            to = (0, 1 - y, zz, r)
            r1[k][to] = (wide(r1[k], *to) + (wide(r0[k], *at) + wide(own[k], *at))).astype(BF)

        rows(k, 2, first)
        stages[k]["a2"] = go(remote(k, 3, r1[k].at[0, 1 - y], r2[k].at[0], py))
        stages[k]["b1"].wait_recv()

        def second(zz, r, k=k):
            at = (1 - x, y, 1, zz, r)
            to = (1, 1 - x, zz, r)
            r1[k][to] = (wide(r1[k], *to) + (wide(r0[k], *at) + wide(own[k], *at))).astype(BF)

        rows(k, 2, second)
        stages[k]["b2"] = go(remote(k, 4, r1[k].at[1, 1 - x], r2[k].at[1], px))

    def so_far(k, h, zz, r):
        at = (x, y, h, zz, r)
        return wide(r2[k], h, zz, r) + wide(r1[k], h, y * (1 - h) + x * h, zz, r) + (wide(r0[k], *at) + wide(own[k], *at))

    for k in range(n):
        stages[k]["a2"].wait_recv()
        stages[k]["b2"].wait_recv()

        def third(i, r, k=k):
            to = (z + 1 + i) % 4
            h, zz = to // 2, to % 2
            r2[k][h, zz, r] = so_far(k, h, zz, r).astype(BF)

        rows(k, 3, third)
        for d in (1, 2, 3):
            to = (z + d) % 4
            stages[k]["z", d] = go(remote(k, 4 + d, r2[k].at[to // 2, to % 2], r3[k].at[d - 1], pz[d - 1]))

    for k in range(n):
        (height, _), t, layer = CHUNKS[k]
        for d in (1, 2, 3):
            stages[k]["z", d].wait_recv()
        h, zz = z // 2, z % 2
        for at in range(0, height, 16):
            some = min(16, ms[t].shape[1] - at)
            r = pl.ds(at, 16)
            g = so_far(k, h, zz, r) + wide(r3[k], 0, r) + wide(r3[k], 1, r) + wide(r3[k], 2, r)
            g = g.astype(BF).astype(F32)[:some]
            e = pl.ds(at, some)
            m = 0.9 * ms[t][layer, e] + 0.1 * g
            v = 0.95 * vs[t][layer, e] + 0.05 * g * g
            mo[t][layer, e] = m
            vo[t][layer, e] = v
            w = ws[t][layer, e].astype(F32)
            w = w - 0.02 * (m * lax.rsqrt(v + 1e-8) + 0.1 * w)
            if some < 16:
                w = jnp.concatenate([w, jnp.zeros((16 - some, w.shape[1]), F32)], axis=0)
            new[k][r] = w.astype(BF)
        stages[k]["put"] = pltpu.make_async_copy(new[k], outs[k].at[x, y, h, zz, c], local_sem.at[k, 1])
        stages[k]["put"].start()
        for d in (1, 2, 3):
            stages[k]["gz", d] = go(remote(k, 7 + d, new[k], outs[k].at[x, y, h, zz, c], pz[d - 1]))

    def up_one(k):
        stages[k]["put"].wait()
        for d in (1, 2, 3):
            stages[k]["gz", d].wait_recv()
        o = outs[k]
        stages[k]["ga2"] = go(remote(k, 11, o.at[x, y, 0, :, c], o.at[x, y, 0, :, c], py))
        stages[k]["gb2"] = go(remote(k, 12, o.at[x, y, 1, :, c], o.at[x, y, 1, :, c], px))

    def up_two(k):
        o = outs[k]
        stages[k]["ga2"].wait_recv()
        stages[k]["ga1"] = go(remote(k, 13, o.at[x, :, 0, :, c], o.at[x, :, 0, :, c], px))
        stages[k]["gb2"].wait_recv()
        stages[k]["gb1"] = go(remote(k, 14, o.at[:, y, 1, :, c], o.at[:, y, 1, :, c], py))

    def up_three(k):
        o = outs[k]
        stages[k]["ga1"].wait_recv()
        stages[k]["gb1"].wait_recv()
        stages[k]["gc"] = go(remote(k, 15, o.at[:, :, :, :, c], o.at[:, :, :, :, c], core))

    for k in range(n):
        up_one(k)
        if k >= 1:
            up_two(k - 1)
        if k >= 2:
            up_three(k - 2)
    up_two(n - 1)
    up_three(n - 2)
    up_three(n - 1)
    for k in range(n):
        stages[k]["gc"].wait_recv()
    for copy in sent:
        copy.wait_send()


def sum_and_step(grads, ws, ms, vs):
    n = len(CHUNKS)
    anywhere, vmem = pl.BlockSpec(memory_space=pl.ANY), pl.BlockSpec(memory_space=pltpu.VMEM)
    blocks = [jax.ShapeDtypeStruct((2, 2, 2, 2, 2, *shape), BF) for shape, _, _ in CHUNKS]
    grads = [g.reshape(b.shape) for g, b in zip(grads, blocks, strict=True)]

    def held(*lead):
        return [pltpu.VMEM((*lead, *shape), BF) for shape, _, _ in CHUNKS]

    done = pl.pallas_call(
        exchange,
        out_shape=[*blocks, *(jax.ShapeDtypeStruct(t.shape, F32) for t in (*ms, *vs))],
        in_specs=[anywhere] * n + [vmem] * 9,
        out_specs=[anywhere] * n + [vmem] * 6,
        scratch_shapes=[
            *held(2, 2, 2, 2), *held(2, 2, 2, 2), *held(2, 2, 2), *held(2, 2), *held(3), *held(),
            pltpu.SemaphoreType.DMA((n, 2)), pltpu.SemaphoreType.DMA((n, 16)), pltpu.SemaphoreType.DMA((n, 16)),
        ],
        compiler_params=pltpu.CompilerParams(collective_id=0, has_side_effects=True, vmem_limit_bytes=67043328),
    )(*grads, *ws, *ms, *vs)
    return done[:n], done[n : n + 3], done[n + 3 :]


def solution(mesh):
    def step(x, dy, wg, wu, wd, mg, mu, md, vg, vu, vd):
        grads = gradients(x[0], dy[0], wg, wu, wd)
        me = lax.axis_index("dp")
        ws = [lax.dynamic_slice_in_dim(w, me * rows, rows, 1) for w, rows in ((wg, 28), (wu, 28), (wd, 80))]
        new, m, v = sum_and_step(grads, ws, (mg, mu, md), (vg, vu, vd))
        d1, g1, u1, d0, g0, u0 = new

        def packed(a, b):
            return jnp.stack([t.reshape(32, 32, 2560)[:, :28].reshape(896, 2560) for t in (a, b)])

        down = jnp.stack([t.reshape(2560, 896) for t in (d0, d1)])
        return (packed(g0, g1), packed(u0, u1), down, *m, *v)

    rows = P(None, "dp", None)
    return jax.shard_map(
        step,
        mesh=mesh,
        in_specs=(P(("rep", "dp")), P(("rep", "dp")), P(), P(), P(), *[rows] * 6),
        out_specs=(*[P("rep")] * 3, *[P("rep", "dp", None)] * 6),
        check_vma=False,
    )
```

```python
import functools

import jax
import jax.numpy as jnp
from jax import lax
from jax.experimental import pallas as pl
from jax.experimental.pallas import tpu as pltpu
from jax.sharding import PartitionSpec as P

F32, BF = jnp.float32, jnp.bfloat16
MESH = pl.DeviceIdType.MESH
WIDE, TALL = (32, 2560), (80, 896)


def dot(a, b, ca, cb):
    return lax.dot_general(a, b, (((ca,), (cb,)), ((), ())), preferred_element_type=F32)


def normed(h):
    wide = h.astype(F32)
    scale = lax.rsqrt(jnp.mean(wide**2, -1, keepdims=True) + 1e-6)
    return (wide * scale).astype(BF), scale


def spread():
    row, f = lax.broadcasted_iota(jnp.int32, (1024, 896), 0), lax.broadcasted_iota(jnp.int32, (1024, 896), 1)
    block = f // 28
    return (512 * (block % 2) + 32 * (block // 2) + f % 28 == row).astype(BF)


TOKENS, PIECE, COLUMNS = 256, 1280, 256


def by_columns(ref, piece, value):
    for at in range(0, PIECE, COLUMNS):
        ref[(piece.start + at) // COLUMNS] = value[:, at : at + COLUMNS]


def states(x_ref, dy_ref, place_ref, wg_ref, wu_ref, wd_ref, b0_ref, p0_ref, dg0_ref, du0_ref, dh_ref, b1_ref, p1_ref, dg1_ref, du1_ref, by_g, by_u):
    pieces = [pl.ds(at, PIECE) for at in range(0, 2560, PIECE)]
    x = x_ref[...]
    a, _ = normed(x)
    b0_ref[...] = dot(place_ref[...], a, 1, 1).astype(BF)
    out = jnp.zeros(x.shape, F32)
    for piece in pieces:
        g, u = dot(a, wg_ref[0, :, piece], 1, 0), dot(a, wu_ref[0, :, piece], 1, 0)
        s = jax.nn.sigmoid(g)
        by_g[:, piece] = u * (s * (1 + g * (1 - s)))
        by_u[:, piece] = g * s
        p = (g * s * u).astype(BF)
        p0_ref[:, piece] = p
        out += dot(p, wd_ref[0, piece], 1, 0)
    h = x + out.astype(BF)
    a, scale = normed(h)
    b1_ref[...] = dot(place_ref[...], a, 1, 1).astype(BF)
    dy = dy_ref[...]
    da = jnp.zeros(x.shape, F32)
    for piece in pieces:
        g, u = dot(a, wg_ref[1, :, piece], 1, 0), dot(a, wu_ref[1, :, piece], 1, 0)
        dp = dot(dy, wd_ref[1, piece], 1, 1).astype(BF).astype(F32)
        s = jax.nn.sigmoid(g)
        p1_ref[:, piece] = (g * s * u).astype(BF)
        dg = (dp * (u * (s * (1 + g * (1 - s))))).astype(BF)
        du = (dp * (g * s)).astype(BF)
        by_columns(dg1_ref, piece, dg)
        by_columns(du1_ref, piece, du)
        da += dot(dg, wg_ref[1, :, piece], 1, 1) + dot(du, wu_ref[1, :, piece], 1, 1)
    unit = h.astype(F32) * scale
    dh = dy + (scale * (da - unit * jnp.mean(da * unit, -1, keepdims=True))).astype(BF)
    dh_ref[...] = dh
    for piece in pieces:
        dp = dot(dh, wd_ref[0, piece], 1, 1).astype(BF).astype(F32)
        by_columns(dg0_ref, piece, (dp * by_g[:, piece]).astype(BF))
        by_columns(du0_ref, piece, (dp * by_u[:, piece]).astype(BF))


def gradients(x, dy, wg, wu, wd):
    n = x.shape[0]

    def block(width):
        return pl.BlockSpec((TOKENS, width), lambda i: (i, 0))

    def whole(t):
        return pl.BlockSpec(t.shape, lambda i: (0,) * t.ndim, pipeline_mode=pl.Buffered(1))

    place = spread()
    tall = pl.BlockSpec((1024, TOKENS), lambda i: (0, i))
    tiles = 2560 // COLUMNS
    tiled = pl.BlockSpec((tiles, TOKENS, COLUMNS), lambda i: (0, i, 0))
    wide = [jax.ShapeDtypeStruct((n, 2560), BF), *[jax.ShapeDtypeStruct((tiles, n, COLUMNS), BF)] * 2]
    spread_out = jax.ShapeDtypeStruct((1024, n), BF)
    b0, p0, dg0, du0, dh, b1, p1, dg1, du1 = pl.pallas_call(
        states,
        grid=(n // TOKENS,),
        out_shape=[spread_out, *wide, jax.ShapeDtypeStruct((n, 896), BF), spread_out, *wide],
        in_specs=[block(896), block(896), *map(whole, (place, wg, wu, wd))],
        out_specs=[tall, block(2560), tiled, tiled, block(896), tall, block(2560), tiled, tiled],
        scratch_shapes=[pltpu.VMEM((TOKENS, 2560), F32)] * 2,
        compiler_params=pltpu.CompilerParams(vmem_limit_bytes=67043328),
        cost_estimate=pl.CostEstimate(flops=92 * 10**9, bytes_accessed=10**8, transcendentals=10**7),
    )(x, dy, place, wg, wu, wd)
    downs = [dot(a, b, 0, 0).astype(BF) for a, b in ((p1, dy), (p0, dh))]
    return downs, [b.reshape(2, 512, n) for b in (b1, b0)], (dg1, du1, dg0, du0)


CHUNKS = [(TALL, 2, 1), (TALL, 2, 0), (WIDE, 0, 1), (WIDE, 1, 1), (WIDE, 0, 0), (WIDE, 1, 0)]


STARTS = (0, 1, 3, 5, 7, 9)
SHARES = {(2, 0): (0, 3), (2, 2): (3, 5), (1, 1): (5, 8), (1, 3): (8, 10)}


def exchange(*refs):
    n = len(CHUNKS)
    downs, lefts, rights, ws, ms, vs = refs[:2], refs[2:4], refs[4:8], refs[8:11], refs[11:14], refs[14:17]
    result, mo, vo = refs[17:20], refs[20:23], refs[23:26]
    outs = [result[t].at[layer] for _, t, layer in CHUNKS]
    scratch = refs[26:]
    own, r0, r1, r2, r3, new = (scratch[i * n : (i + 1) * n] for i in range(6))
    local_sem, send_sem, recv_sem, left, right, stage_out, left_sem, right_sem, stage_sem = scratch[6 * n :]

    me = lax.axis_index("dp")
    c, z, y, x = me % 2, (me // 2) % 4, (me // 8) % 2, me // 16
    core, px, py = me + 1 - 2 * c, me + 16 - 32 * x, me + 8 - 16 * y
    pz = [me + 2 * ((z + d) % 4 - z) for d in (1, 2, 3)]

    barrier = pltpu.get_barrier_semaphore()
    for peer in (core, px, py, *pz):
        pl.semaphore_signal(barrier, inc=1, device_id={"dp": peer}, device_id_type=MESH)
    pl.semaphore_wait(barrier, 6)

    def remote(k, slot, src, dst, peer):
        return pltpu.make_async_remote_copy(
            src_ref=src, dst_ref=dst, send_sem=send_sem.at[k, slot], recv_sem=recv_sem.at[k, slot],
            device_id={"dp": peer}, device_id_type=MESH,
        )

    def rows(k, blocks, body):
        per = CHUNKS[k][0][0] // 16

        def step(i, _):
            body(i // per, pl.ds(pl.multiple_of(i % per * 16, 16), 16))
            return 0

        lax.fori_loop(0, blocks * per, step, 0)

    def wide(ref, *at):
        return ref[at].astype(F32)

    sent = []

    def go(copy):
        copy.start()
        sent.append(copy)
        return copy

    stages = [{} for _ in range(n)]
    for k in range(2):
        stages[k]["own"] = pltpu.make_async_copy(downs[k].at[:, :, :, :, c], own[k], local_sem.at[k, 0])
        stages[k]["own"].start()
        stages[k]["core"] = go(remote(k, 0, downs[k].at[:, :, :, :, 1 - c], r0[k], core))

    def left_copy(i):
        return pltpu.make_async_copy(lefts[i], left, left_sem)

    left_copy(0).start()
    tiles = 2560 // COLUMNS

    def columns(j):
        return pl.ds(pl.multiple_of(j * COLUMNS, COLUMNS), COLUMNS)

    def right_copy(k, j):
        return pltpu.make_async_copy(rights[k - 2].at[j], right.at[j % 3], right_sem.at[j % 3])

    def core_copy(k, j):
        return pltpu.make_async_remote_copy(
            src_ref=stage_out.at[j % 2], dst_ref=r0[k].at[:, :, :, :, :, columns(j)],
            send_sem=stage_sem.at[j % 2], recv_sem=recv_sem.at[k, 0],
            device_id={"dp": core}, device_id_type=MESH,
        )

    def multiply(k, begin, end):
        if begin == 0:
            if k % 2 == 0:
                left_copy(k // 2 - 1).wait()
            right_copy(k, 0).start()
            right_copy(k, 1).start()

        def tile(j, _):
            @pl.when(j + 2 < tiles)
            def _():
                right_copy(k, j + 2).start()

            right_copy(k, j).wait()

            @pl.when(j >= 2)
            def _():
                core_copy(k, j).wait_send()

            b = right[j % 3]
            stage_out[j % 2] = dot(left[1 - c], b, 1, 0).astype(BF).reshape(2, 2, 2, 2, 32, COLUMNS)
            core_copy(k, j).start()
            own[k][:, :, :, :, :, columns(j)] = dot(left[c], b, 1, 0).astype(BF).reshape(2, 2, 2, 2, 32, COLUMNS)
            return 0

        lax.fori_loop(begin, end, tile, 0)
        if end < tiles:
            return
        for j in (tiles - 2, tiles - 1):
            core_copy(k, j).wait_send()
        if k == 3:
            left_copy(1).start()

    def down_one(k):
        if k < 2:
            stages[k]["own"].wait()
        remote(k, 0, r0[k], r0[k], core).wait_recv()

        def first(i, r, k=k):
            q, zz = i // 2, i % 2
            at = (1 - x, q, 0, zz, r)
            r0[k][at] = (wide(r0[k], *at) + wide(own[k], *at)).astype(BF)

        rows(k, 4, first)
        stages[k]["a1"] = go(remote(k, 1, r0[k].at[1 - x, :, 0], r1[k].at[0], px))

        def second(i, r, k=k):
            q, zz = i // 2, i % 2
            at = (q, 1 - y, 1, zz, r)
            r0[k][at] = (wide(r0[k], *at) + wide(own[k], *at)).astype(BF)

        rows(k, 4, second)
        stages[k]["b1"] = go(remote(k, 2, r0[k].at[:, 1 - y, 1], r1[k].at[1], py))

    def down_two(k):
        stages[k]["a1"].wait_recv()

        def first(zz, r, k=k):
            at = (x, 1 - y, 0, zz, r)
            to = (0, 1 - y, zz, r)
            r1[k][to] = (wide(r1[k], *to) + (wide(r0[k], *at) + wide(own[k], *at))).astype(BF)

        rows(k, 2, first)
        stages[k]["a2"] = go(remote(k, 3, r1[k].at[0, 1 - y], r2[k].at[0], py))
        stages[k]["b1"].wait_recv()

        def second(zz, r, k=k):
            at = (1 - x, y, 1, zz, r)
            to = (1, 1 - x, zz, r)
            r1[k][to] = (wide(r1[k], *to) + (wide(r0[k], *at) + wide(own[k], *at))).astype(BF)

        rows(k, 2, second)
        stages[k]["b2"] = go(remote(k, 4, r1[k].at[1, 1 - x], r2[k].at[1], px))

    def so_far(k, h, zz, r):
        at = (x, y, h, zz, r)
        return wide(r2[k], h, zz, r) + wide(r1[k], h, y * (1 - h) + x * h, zz, r) + (wide(r0[k], *at) + wide(own[k], *at))

    def down_three(k):
        stages[k]["a2"].wait_recv()
        stages[k]["b2"].wait_recv()

        def third(i, r, k=k):
            to = (z + 1 + i) % 4
            h, zz = to // 2, to % 2
            r2[k][h, zz, r] = so_far(k, h, zz, r).astype(BF)

        rows(k, 3, third)
        for d in (1, 2, 3):
            to = (z + d) % 4
            stages[k]["z", d] = go(remote(k, 4 + d, r2[k].at[to // 2, to % 2], r3[k].at[d - 1], pz[d - 1]))

    def take(k):
        (height, _), t, layer = CHUNKS[k]
        for d in (1, 2, 3):
            stages[k]["z", d].wait_recv()
        h, zz = z // 2, z % 2
        for at in range(0, height, 16):
            some = min(16, ws[t].shape[1] - at)
            r = pl.ds(at, 16)
            g = so_far(k, h, zz, r) + wide(r3[k], 0, r) + wide(r3[k], 1, r) + wide(r3[k], 2, r)
            g = g.astype(BF).astype(F32)[:some]
            e = pl.ds(at, some)
            at_mv = (layer, e) if t == 2 else (e, layer)
            m = 0.9 * ms[t][at_mv] + 0.1 * g
            v = 0.95 * vs[t][at_mv] + 0.05 * g * g
            mo[t][at_mv] = m
            vo[t][at_mv] = v
            w = ws[t][layer, e].astype(F32)
            w = w - 0.02 * (m * lax.rsqrt(v + 1e-8) + 0.1 * w)
            if some < 16:
                w = jnp.concatenate([w, jnp.zeros((16 - some, w.shape[1]), F32)], axis=0)
            new[k][r] = w.astype(BF)
        stages[k]["put"] = pltpu.make_async_copy(new[k], outs[k].at[x, y, h, zz, c], local_sem.at[k, 1])
        stages[k]["put"].start()
        for d in (1, 2, 3):
            stages[k]["gz", d] = go(remote(k, 7 + d, new[k], outs[k].at[x, y, h, zz, c], pz[d - 1]))

    def up_one(k):
        stages[k]["put"].wait()
        for d in (1, 2, 3):
            stages[k]["gz", d].wait_recv()
        o = outs[k]
        stages[k]["ga2"] = go(remote(k, 11, o.at[x, y, 0, :, c], o.at[x, y, 0, :, c], py))
        stages[k]["gb2"] = go(remote(k, 12, o.at[x, y, 1, :, c], o.at[x, y, 1, :, c], px))

    def up_two(k):
        o = outs[k]
        stages[k]["ga2"].wait_recv()
        stages[k]["ga1"] = go(remote(k, 13, o.at[x, :, 0, :, c], o.at[x, :, 0, :, c], px))
        stages[k]["gb2"].wait_recv()
        stages[k]["gb1"] = go(remote(k, 14, o.at[:, y, 1, :, c], o.at[:, y, 1, :, c], py))

    def up_three(k):
        o = outs[k]
        stages[k]["ga1"].wait_recv()
        stages[k]["gb1"].wait_recv()
        stages[k]["gc"] = go(remote(k, 15, o.at[:, :, :, :, c], o.at[:, :, :, :, c], core))

    def finish(k):
        stages[k]["gc"].wait_recv()

    order = (down_one, down_two, down_three, take, up_one, up_two, up_three, finish)
    starts = STARTS
    for now in range(starts[-1] + len(order)):
        for lag, stage in enumerate(order):
            for k in range(n):
                if now - starts[k] == lag:
                    stage(k)
            for k in range(2, n):
                if (starts[k] - now, lag) in SHARES:
                    multiply(k, *SHARES[starts[k] - now, lag])
    for copy in sent:
        copy.wait_send()


def sum_and_step(downs, lefts, rights, ws, ms, vs):
    n = len(CHUNKS)
    anywhere, vmem = pl.BlockSpec(memory_space=pl.ANY), pl.BlockSpec(memory_space=pltpu.VMEM)
    results = [jax.ShapeDtypeStruct((2, 2, 2, 2, 2, 2, *shape), BF) for shape in (WIDE, WIDE, TALL)]
    downs = [g.reshape(2, 2, 2, 2, 2, *TALL) for g in downs]
    tokens = lefts[0].shape[2]

    def held(*lead):
        return [pltpu.VMEM((*lead, *shape), BF) for shape, _, _ in CHUNKS]

    done = pl.pallas_call(
        exchange,
        out_shape=[*results, *(jax.ShapeDtypeStruct(t.shape, F32) for t in (*ms, *vs))],
        in_specs=[anywhere] * 8 + [vmem] * 9,
        out_specs=[anywhere] * 3 + [vmem] * 6,
        scratch_shapes=[
            *held(2, 2, 2, 2), *held(2, 2, 2, 2), *held(2, 2, 2), *held(2, 2), *held(3), *held(),
            pltpu.SemaphoreType.DMA((n, 2)), pltpu.SemaphoreType.DMA((n, 16)), pltpu.SemaphoreType.DMA((n, 16)),
            pltpu.VMEM((2, 512, tokens), BF), pltpu.VMEM((3, tokens, COLUMNS), BF), pltpu.VMEM((2, 2, 2, 2, 2, 32, COLUMNS), BF),
            pltpu.SemaphoreType.DMA, pltpu.SemaphoreType.DMA((3,)), pltpu.SemaphoreType.DMA((2,)),
        ],
        compiler_params=pltpu.CompilerParams(collective_id=0, has_side_effects=True, vmem_limit_bytes=67043328),
    )(*downs, *lefts, *rights, *ws, *ms, *vs)
    return done[:3], done[3:6], done[6:]


def gather_rows(from_ref, to_ref):
    for i in range(8):
        to_ref[0, 28 * i : 28 * i + 28] = from_ref[0, i, :28]


def packed(t):
    return pl.pallas_call(
        gather_rows,
        grid=(2, 4),
        out_shape=jax.ShapeDtypeStruct((2, 896, 2560), BF),
        in_specs=[pl.BlockSpec((1, 8, 32, 2560), lambda i, j: (i, j, 0, 0))],
        out_specs=pl.BlockSpec((1, 224, 2560), lambda i, j: (i, j, 0)),
    )(t.reshape(2, 32, 32, 2560))


def solution(mesh):
    def step(x, dy, wg, wu, wd, mg, mu, md, vg, vu, vd):
        terms = gradients(x[0], dy[0], wg, wu, wd)
        me = lax.axis_index("dp")
        ws = [lax.dynamic_slice_in_dim(w, me * rows, rows, 1) for w, rows in ((wg, 28), (wu, 28), (wd, 80))]
        swap = lambda ts: [*(t.swapaxes(0, 1) for t in ts[:2]), ts[2]]
        new, m, v = sum_and_step(*terms, ws, swap((mg, mu, md)), swap((vg, vu, vd)))
        m, v = swap(m), swap(v)
        gate, up, down = new
        return (packed(gate), packed(up), down.reshape(2, 2560, 896), *m, *v)

    rows = P(None, "dp", None)
    return jax.shard_map(
        step,
        mesh=mesh,
        in_specs=(P(("rep", "dp")), P(("rep", "dp")), P(), P(), P(), *[rows] * 6),
        out_specs=(*[P("rep")] * 3, *[P("rep", "dp", None)] * 6),
        check_vma=False,
    )
```

```python
import functools

import jax
import jax.numpy as jnp
from jax import lax
from jax.experimental import pallas as pl
from jax.experimental.pallas import tpu as pltpu
from jax.sharding import PartitionSpec as P

F32, BF = jnp.float32, jnp.bfloat16
MESH = pl.DeviceIdType.MESH
WIDE, TALL = (32, 2560), (80, 896)


def dot(a, b, ca, cb):
    return lax.dot_general(a, b, (((ca,), (cb,)), ((), ())), preferred_element_type=F32)


def normed(h):
    wide = h.astype(F32)
    scale = lax.rsqrt(jnp.mean(wide**2, -1, keepdims=True) + 1e-6)
    return (wide * scale).astype(BF), scale


def spread():
    row, f = lax.broadcasted_iota(jnp.int32, (1024, 896), 0), lax.broadcasted_iota(jnp.int32, (1024, 896), 1)
    block = f // 28
    return (512 * (block % 2) + 32 * (block // 2) + f % 28 == row).astype(BF)


TOKENS, PIECE, COLUMNS = 256, 2560, 256


def by_columns(ref, piece, value):
    for at in range(0, PIECE, COLUMNS):
        ref[(piece.start + at) // COLUMNS] = value[:, at : at + COLUMNS]


def states(x_ref, dy_ref, place_ref, wg_ref, wu_ref, wd_ref, b0_ref, p0_ref, dg0_ref, du0_ref, dh_ref, b1_ref, p1_ref, dg1_ref, du1_ref, by_g, by_u):
    pieces = [pl.ds(at, PIECE) for at in range(0, 2560, PIECE)]
    x = x_ref[...]
    a, _ = normed(x)
    b0_ref[...] = dot(place_ref[...], a, 1, 1).astype(BF)
    out = jnp.zeros(x.shape, F32)
    for piece in pieces:
        g, u = dot(a, wg_ref[0, :, piece], 1, 0), dot(a, wu_ref[0, :, piece], 1, 0)
        s = jax.nn.sigmoid(g)
        by_g[:, piece] = u * (s * (1 + g * (1 - s)))
        by_u[:, piece] = g * s
        p = (g * s * u).astype(BF)
        p0_ref[:, piece] = p
        out += dot(p, wd_ref[0, piece], 1, 0)
    h = x + out.astype(BF)
    a, scale = normed(h)
    b1_ref[...] = dot(place_ref[...], a, 1, 1).astype(BF)
    dy = dy_ref[...]
    da = jnp.zeros(x.shape, F32)
    for piece in pieces:
        g, u = dot(a, wg_ref[1, :, piece], 1, 0), dot(a, wu_ref[1, :, piece], 1, 0)
        dp = dot(dy, wd_ref[1, piece], 1, 1).astype(BF).astype(F32)
        s = jax.nn.sigmoid(g)
        p1_ref[:, piece] = (g * s * u).astype(BF)
        dg = (dp * (u * (s * (1 + g * (1 - s))))).astype(BF)
        du = (dp * (g * s)).astype(BF)
        by_columns(dg1_ref, piece, dg)
        by_columns(du1_ref, piece, du)
        da += dot(dg, wg_ref[1, :, piece], 1, 1) + dot(du, wu_ref[1, :, piece], 1, 1)
    unit = h.astype(F32) * scale
    dh = dy + (scale * (da - unit * jnp.mean(da * unit, -1, keepdims=True))).astype(BF)
    dh_ref[...] = dh
    for piece in pieces:
        dp = dot(dh, wd_ref[0, piece], 1, 1).astype(BF).astype(F32)
        by_columns(dg0_ref, piece, (dp * by_g[:, piece]).astype(BF))
        by_columns(du0_ref, piece, (dp * by_u[:, piece]).astype(BF))


def gradients(x, dy, wg, wu, wd):
    n = x.shape[0]

    def block(width):
        return pl.BlockSpec((TOKENS, width), lambda i: (i, 0))

    def whole(t):
        return pl.BlockSpec(t.shape, lambda i: (0,) * t.ndim, pipeline_mode=pl.Buffered(1))

    place = spread()
    tall = pl.BlockSpec((1024, TOKENS), lambda i: (0, i))
    tiles = 2560 // COLUMNS
    tiled = pl.BlockSpec((tiles, TOKENS, COLUMNS), lambda i: (0, i, 0))
    wide = [jax.ShapeDtypeStruct((n, 2560), BF), *[jax.ShapeDtypeStruct((tiles, n, COLUMNS), BF)] * 2]
    spread_out = jax.ShapeDtypeStruct((1024, n), BF)
    b0, p0, dg0, du0, dh, b1, p1, dg1, du1 = pl.pallas_call(
        states,
        grid=(n // TOKENS,),
        out_shape=[spread_out, *wide, jax.ShapeDtypeStruct((n, 896), BF), spread_out, *wide],
        in_specs=[block(896), block(896), *map(whole, (place, wg, wu, wd))],
        out_specs=[tall, block(2560), tiled, tiled, block(896), tall, block(2560), tiled, tiled],
        scratch_shapes=[pltpu.VMEM((TOKENS, 2560), F32)] * 2,
        compiler_params=pltpu.CompilerParams(vmem_limit_bytes=67043328),
        cost_estimate=pl.CostEstimate(flops=92 * 10**9, bytes_accessed=10**8, transcendentals=10**7),
    )(x, dy, place, wg, wu, wd)
    downs = [dot(a, b, 0, 0).astype(BF) for a, b in ((p1, dy), (p0, dh))]
    return downs, [b.reshape(2, 512, n) for b in (b1, b0)], (dg1, du1, dg0, du0)


CHUNKS = [(TALL, 2, 1), (TALL, 2, 0), (WIDE, 0, 1), (WIDE, 1, 1), (WIDE, 0, 0), (WIDE, 1, 0)]


STARTS = (0, 1, 3, 5, 7, 9)
SHARES = {(2, 0): (0, 3), (2, 2): (3, 5), (1, 1): (5, 8), (1, 3): (8, 10)}


def exchange(*refs):
    n = len(CHUNKS)
    downs, lefts, rights, ws, ms, vs = refs[:2], refs[2:4], refs[4:8], refs[8:11], refs[11:14], refs[14:17]
    result, mo, vo = refs[17:20], refs[20:23], refs[23:26]
    outs = [result[t].at[layer] for _, t, layer in CHUNKS]
    scratch = refs[26:]
    own, r0, r1, r2, r3, new = (scratch[i * n : (i + 1) * n] for i in range(6))
    local_sem, send_sem, recv_sem, left, right, stage_out, left_sem, right_sem, stage_sem = scratch[6 * n :]

    me = lax.axis_index("dp")
    c, z, y, x = me % 2, (me // 2) % 4, (me // 8) % 2, me // 16
    core, px, py = me + 1 - 2 * c, me + 16 - 32 * x, me + 8 - 16 * y
    pz = [me + 2 * ((z + d) % 4 - z) for d in (1, 2, 3)]

    barrier = pltpu.get_barrier_semaphore()
    for peer in (core, px, py, *pz):
        pl.semaphore_signal(barrier, inc=1, device_id={"dp": peer}, device_id_type=MESH)
    pl.semaphore_wait(barrier, 6)

    def remote(k, slot, src, dst, peer):
        return pltpu.make_async_remote_copy(
            src_ref=src, dst_ref=dst, send_sem=send_sem.at[k, slot], recv_sem=recv_sem.at[k, slot],
            device_id={"dp": peer}, device_id_type=MESH,
        )

    def rows(k, blocks, body):
        height = CHUNKS[k][0][0]
        some = 32 if height == 32 else 80
        per = height // some

        def step(i, _):
            body(i // per, pl.ds(pl.multiple_of(i % per * some, 16), some))
            return 0

        lax.fori_loop(0, blocks * per, step, 0)

    def wide(ref, *at):
        return ref[at].astype(F32)

    sent = []

    def go(copy):
        copy.start()
        sent.append(copy)
        return copy

    stages = [{} for _ in range(n)]
    for k in range(2):
        stages[k]["own"] = pltpu.make_async_copy(downs[k].at[:, :, :, :, c], own[k], local_sem.at[k, 0])
        stages[k]["own"].start()
        stages[k]["core"] = go(remote(k, 0, downs[k].at[:, :, :, :, 1 - c], r0[k], core))

    def left_copy(i):
        return pltpu.make_async_copy(lefts[i], left, left_sem)

    left_copy(0).start()
    tiles = 2560 // COLUMNS

    def columns(j):
        return pl.ds(pl.multiple_of(j * COLUMNS, COLUMNS), COLUMNS)

    def right_copy(k, j):
        return pltpu.make_async_copy(rights[k - 2].at[j], right.at[j % 3], right_sem.at[j % 3])

    def core_copy(k, j):
        return pltpu.make_async_remote_copy(
            src_ref=stage_out.at[j % 2], dst_ref=r0[k].at[:, :, :, :, :, columns(j)],
            send_sem=stage_sem.at[j % 2], recv_sem=recv_sem.at[k, 0],
            device_id={"dp": core}, device_id_type=MESH,
        )

    def multiply(k, begin, end):
        if begin == 0:
            if k % 2 == 0:
                left_copy(k // 2 - 1).wait()
            right_copy(k, 0).start()
            right_copy(k, 1).start()

        def tile(j, _):
            @pl.when(j + 2 < tiles)
            def _():
                right_copy(k, j + 2).start()

            right_copy(k, j).wait()

            @pl.when(j >= 2)
            def _():
                core_copy(k, j).wait_send()

            b = right[j % 3]
            stage_out[j % 2] = dot(left[1 - c], b, 1, 0).astype(BF).reshape(2, 2, 2, 2, 32, COLUMNS)
            core_copy(k, j).start()
            own[k][:, :, :, :, :, columns(j)] = dot(left[c], b, 1, 0).astype(BF).reshape(2, 2, 2, 2, 32, COLUMNS)
            return 0

        lax.fori_loop(begin, end, tile, 0)
        if end < tiles:
            return
        for j in (tiles - 2, tiles - 1):
            core_copy(k, j).wait_send()
        if k == 3:
            left_copy(1).start()

    def down_one(k):
        if k < 2:
            stages[k]["own"].wait()
        remote(k, 0, r0[k], r0[k], core).wait_recv()

        def first(i, r, k=k):
            q, zz = i // 2, i % 2
            at = (1 - x, q, 0, zz, r)
            r0[k][at] = (wide(r0[k], *at) + wide(own[k], *at)).astype(BF)

        rows(k, 4, first)
        stages[k]["a1"] = go(remote(k, 1, r0[k].at[1 - x, :, 0], r1[k].at[0], px))

        def second(i, r, k=k):
            q, zz = i // 2, i % 2
            at = (q, 1 - y, 1, zz, r)
            r0[k][at] = (wide(r0[k], *at) + wide(own[k], *at)).astype(BF)

        rows(k, 4, second)
        stages[k]["b1"] = go(remote(k, 2, r0[k].at[:, 1 - y, 1], r1[k].at[1], py))

    def down_two(k):
        stages[k]["a1"].wait_recv()

        def first(zz, r, k=k):
            at = (x, 1 - y, 0, zz, r)
            to = (0, 1 - y, zz, r)
            r1[k][to] = (wide(r1[k], *to) + (wide(r0[k], *at) + wide(own[k], *at))).astype(BF)

        rows(k, 2, first)
        stages[k]["a2"] = go(remote(k, 3, r1[k].at[0, 1 - y], r2[k].at[0], py))
        stages[k]["b1"].wait_recv()

        def second(zz, r, k=k):
            at = (1 - x, y, 1, zz, r)
            to = (1, 1 - x, zz, r)
            r1[k][to] = (wide(r1[k], *to) + (wide(r0[k], *at) + wide(own[k], *at))).astype(BF)

        rows(k, 2, second)
        stages[k]["b2"] = go(remote(k, 4, r1[k].at[1, 1 - x], r2[k].at[1], px))

    def so_far(k, h, zz, r):
        at = (x, y, h, zz, r)
        return wide(r2[k], h, zz, r) + wide(r1[k], h, y * (1 - h) + x * h, zz, r) + (wide(r0[k], *at) + wide(own[k], *at))

    def down_three(k):
        stages[k]["a2"].wait_recv()
        stages[k]["b2"].wait_recv()

        def third(i, r, k=k):
            to = (z + 1 + i) % 4
            h, zz = to // 2, to % 2
            r2[k][h, zz, r] = so_far(k, h, zz, r).astype(BF)

        rows(k, 3, third)
        for d in (1, 2, 3):
            to = (z + d) % 4
            stages[k]["z", d] = go(remote(k, 4 + d, r2[k].at[to // 2, to % 2], r3[k].at[d - 1], pz[d - 1]))

    def take(k):
        (height, _), t, layer = CHUNKS[k]
        for d in (1, 2, 3):
            stages[k]["z", d].wait_recv()
        h, zz = z // 2, z % 2
        for at in range(0, height, 16):
            some = min(16, ws[t].shape[1] - at)
            r = pl.ds(at, 16)
            g = so_far(k, h, zz, r) + wide(r3[k], 0, r) + wide(r3[k], 1, r) + wide(r3[k], 2, r)
            g = g.astype(BF).astype(F32)[:some]
            e = pl.ds(at, some)
            at_mv = (layer, e) if t == 2 else (e, layer)
            m = 0.9 * ms[t][at_mv] + 0.1 * g
            v = 0.95 * vs[t][at_mv] + 0.05 * g * g
            mo[t][at_mv] = m
            vo[t][at_mv] = v
            w = ws[t][layer, e].astype(F32)
            w = w - 0.02 * (m * lax.rsqrt(v + 1e-8) + 0.1 * w)
            if some < 16:
                w = jnp.concatenate([w, jnp.zeros((16 - some, w.shape[1]), F32)], axis=0)
            new[k][r] = w.astype(BF)
        stages[k]["put"] = pltpu.make_async_copy(new[k], outs[k].at[x, y, h, zz, c], local_sem.at[k, 1])
        stages[k]["put"].start()
        for d in (1, 2, 3):
            stages[k]["gz", d] = go(remote(k, 7 + d, new[k], outs[k].at[x, y, h, zz, c], pz[d - 1]))

    def up_one(k):
        stages[k]["put"].wait()
        for d in (1, 2, 3):
            stages[k]["gz", d].wait_recv()
        o = outs[k]
        stages[k]["ga2"] = go(remote(k, 11, o.at[x, y, 0, :, c], o.at[x, y, 0, :, c], py))
        stages[k]["gb2"] = go(remote(k, 12, o.at[x, y, 1, :, c], o.at[x, y, 1, :, c], px))

    def up_two(k):
        o = outs[k]
        stages[k]["ga2"].wait_recv()
        stages[k]["ga1"] = go(remote(k, 13, o.at[x, :, 0, :, c], o.at[x, :, 0, :, c], px))
        stages[k]["gb2"].wait_recv()
        stages[k]["gb1"] = go(remote(k, 14, o.at[:, y, 1, :, c], o.at[:, y, 1, :, c], py))

    def up_three(k):
        o = outs[k]
        stages[k]["ga1"].wait_recv()
        stages[k]["gb1"].wait_recv()
        stages[k]["gc"] = go(remote(k, 15, o.at[:, :, :, :, c], o.at[:, :, :, :, c], core))

    def finish(k):
        stages[k]["gc"].wait_recv()

    order = (down_one, down_two, down_three, take, up_one, up_two, up_three, finish)
    starts = STARTS
    for now in range(starts[-1] + len(order)):
        for lag, stage in enumerate(order):
            for k in range(n):
                if now - starts[k] == lag:
                    stage(k)
            for k in range(2, n):
                if (starts[k] - now, lag) in SHARES:
                    multiply(k, *SHARES[starts[k] - now, lag])
    for copy in sent:
        copy.wait_send()


def sum_and_step(downs, lefts, rights, ws, ms, vs):
    n = len(CHUNKS)
    anywhere, vmem = pl.BlockSpec(memory_space=pl.ANY), pl.BlockSpec(memory_space=pltpu.VMEM)
    results = [jax.ShapeDtypeStruct((2, 2, 2, 2, 2, 2, *shape), BF) for shape in (WIDE, WIDE, TALL)]
    downs = [g.reshape(2, 2, 2, 2, 2, *TALL) for g in downs]
    tokens = lefts[0].shape[2]

    def held(*lead):
        return [pltpu.VMEM((*lead, *shape), BF) for shape, _, _ in CHUNKS]

    done = pl.pallas_call(
        exchange,
        out_shape=[*results, *(jax.ShapeDtypeStruct(t.shape, F32) for t in (*ms, *vs))],
        in_specs=[anywhere] * 8 + [vmem] * 9,
        out_specs=[anywhere] * 3 + [vmem] * 6,
        scratch_shapes=[
            *held(2, 2, 2, 2), *held(2, 2, 2, 2), *held(2, 2, 2), *held(2, 2), *held(3), *held(),
            pltpu.SemaphoreType.DMA((n, 2)), pltpu.SemaphoreType.DMA((n, 16)), pltpu.SemaphoreType.DMA((n, 16)),
            pltpu.VMEM((2, 512, tokens), BF), pltpu.VMEM((3, tokens, COLUMNS), BF), pltpu.VMEM((2, 2, 2, 2, 2, 32, COLUMNS), BF),
            pltpu.SemaphoreType.DMA, pltpu.SemaphoreType.DMA((3,)), pltpu.SemaphoreType.DMA((2,)),
        ],
        compiler_params=pltpu.CompilerParams(collective_id=0, has_side_effects=True, vmem_limit_bytes=67043328),
    )(*downs, *lefts, *rights, *ws, *ms, *vs)
    return done[:3], done[3:6], done[6:]


def gather_rows(from_ref, to_ref):
    for i in range(8):
        to_ref[0, 28 * i : 28 * i + 28] = from_ref[0, i, :28]


def packed(t):
    return pl.pallas_call(
        gather_rows,
        grid=(2, 4),
        out_shape=jax.ShapeDtypeStruct((2, 896, 2560), BF),
        in_specs=[pl.BlockSpec((1, 8, 32, 2560), lambda i, j: (i, j, 0, 0))],
        out_specs=pl.BlockSpec((1, 224, 2560), lambda i, j: (i, j, 0)),
    )(t.reshape(2, 32, 32, 2560))


def solution(mesh):
    def step(x, dy, wg, wu, wd, mg, mu, md, vg, vu, vd):
        terms = gradients(x[0], dy[0], wg, wu, wd)
        me = lax.axis_index("dp")
        ws = [lax.dynamic_slice_in_dim(w, me * rows, rows, 1) for w, rows in ((wg, 28), (wu, 28), (wd, 80))]
        swap = lambda ts: [*(t.swapaxes(0, 1) for t in ts[:2]), ts[2]]
        new, m, v = sum_and_step(*terms, ws, swap((mg, mu, md)), swap((vg, vu, vd)))
        m, v = swap(m), swap(v)
        gate, up, down = new
        return (packed(gate), packed(up), down.reshape(2, 2560, 896), *m, *v)

    rows = P(None, "dp", None)
    return jax.shard_map(
        step,
        mesh=mesh,
        in_specs=(P(("rep", "dp")), P(("rep", "dp")), P(), P(), P(), *[rows] * 6),
        out_specs=(*[P("rep")] * 3, *[P("rep", "dp", None)] * 6),
        check_vma=False,
    )
```
